32 devices in a mesh: clu: 16 (over z, x, core), doc: 2 (over y).
Axes of the slice: x: 2, y: 2, z: 4, core: 2. Of those that a mesh axis runs over, the one named last changes fastest.
Arguments:
- docs: bfloat16 [8192, 768], P(('clu', 'doc')), may hold values from -6 to 6
- centroids: bfloat16 [5504, 768], P('doc', 'clu'), may hold values from -6 to 6
- assigned: int32 [8192], P(('clu', 'doc')), may hold values from 0 to 5503
Outputs:
- nearest: float32 [8192], P(('clu', 'doc'))
- assigned_dist: float32 [8192], P(('clu', 'doc'))
The draws below stay inside these ranges and needn't reach their ends.
Inputs may be any that keep to these rules, and one draw needn't show every extreme that they name: `assigned`: cluster ids.
All inputs are finite; a program needn't handle non-finite values.
Results may differ from the reference program's by a relative error of at most 0.0003.
Values may be sent and summed in bfloat16 or wider, within the bound.
A program may use at most 64 MiB of HBM per device.

```python
import jax
import jax.numpy as jnp
from jax import lax

D = 768
K = 5504
N = 8192
N_CLU = 16


def touch_ends(entries, stream_key, least, top_value):
    longest = entries.shape.index(max(entries.shape))
    spots = []
    for shift in (0, 1):
        where = [jax.random.randint(jax.random.fold_in(stream_key, axis), (), 0, length) for axis, length in enumerate(entries.shape)]
        where[longest] = (where[longest] + shift) % entries.shape[longest]
        spots.append(tuple(where))
    return entries.at[spots[0]].set(least).at[spots[1]].set(top_value)


def block_scale(key, dims, pieces, least, largest):
    def one(dim, blocks):
        steps = jax.random.uniform(jax.random.fold_in(jax.random.fold_in(key, 6), dim), (blocks,), jnp.float32, least / len(pieces), largest / len(pieces))
        return jnp.repeat(jnp.exp(steps), dims[dim] // blocks).reshape((-1,) + (1,) * (len(dims) - dim - 1))

    gain = one(*pieces[0])
    for cut in pieces[1:]:
        gain = gain * one(*cut)
    return gain


def centred(own_key, dims, spread, bound, shards=(), dtype=jnp.bfloat16):
    level = block_scale(own_key, dims, shards, -0.22, 0.18) if shards else 1.0
    values = jax.random.normal(own_key, dims, jnp.float32) * spread * level
    return jnp.minimum(jnp.maximum(values, -bound), bound).astype(dtype)


def setup_inputs(seed: int = 0) -> dict:
    splits = jax.random.split(jax.random.key(seed), 4)
    return {
        "docs": centred(splits[0], (N, D), 1.0, 6.0, ((0, 32),)),
        "centroids": centred(splits[1], (K, D), 1.0, 6.0, ((0, 2), (1, 16))),
        "assigned": touch_ends(jax.random.randint(splits[2], (N,), 0, K), jax.random.fold_in(splits[2], 1), 0, K - 1).astype(jnp.int32),
    }


epsilon = 1e-06

def reference(docs, centroids, assigned):
    cent_wide = centroids.astype(jnp.float32)
    scale_c = lax.rsqrt(lax.optimization_barrier(jnp.sum(cent_wide * cent_wide, 1)) + epsilon)
    features = docs.shape[1]

    def score_block(inputs):
        doc_rows, doc_ids = inputs
        row_wide = doc_rows.astype(jnp.float32)
        scale_x = lax.rsqrt(lax.optimization_barrier(jnp.sum(row_wide * row_wide, 1)) + epsilon)
        products = jnp.dot(doc_rows, centroids.T, preferred_element_type=jnp.float32)
        distance = 1.0 - products * scale_x[:, None] * scale_c[None, :]
        nearest = lax.optimization_barrier(jnp.min(distance, 1))
        chosen = jnp.take_along_axis(distance, doc_ids[:, None].astype(jnp.int32), axis=1)[:, 0]
        return (nearest, chosen)
    nearest, chosen = lax.map(score_block, (docs.reshape(N_CLU, -1, features), assigned.reshape(N_CLU, -1)))
    return (nearest.reshape(-1), chosen.reshape(-1))
```

```python
import functools

import jax
import jax.numpy as jnp
from jax import lax
from jax.experimental import pallas as pl
from jax.experimental.pallas import tpu as pltpu
from jax.sharding import PartitionSpec as P

epsilon = 1e-06
TILE = 256
MESH = pl.DeviceIdType.MESH


def chip_at(pos, n):
    half = n // 2
    return jnp.where(pos < half, 2 * pos, 2 * (n - 1 - pos) + 1)


def kernel(n, nd, feat, docs_in, cents_in, ids_in, near_out, chosen_out,
           buf, docs_all, ids_all, dp_a, dp_b, dp_c, acc, idb, mx, ch, csq, scale, res, got,
           local_sem, ring_send, pair_send, recv, docs_send, docs_recv, ids_send, ids_recv,
           res_send, res_recv):
    hops = n // 2
    fp = cents_in.shape[0]
    width = cents_in.shape[1]
    rows_dev = docs_in.shape[0]
    cut = (width // 2 + 127) // 128 * 128
    chunks = ((0, cut), (cut, width - cut))

    clu, doc = lax.axis_index("clu"), lax.axis_index("doc")
    core, chip = lax.rem(clu, 2), lax.div(clu, 2)
    z, x = lax.div(chip, 2), lax.rem(chip, 2)
    pos = jnp.where(x == 0, z, n - 1 - z)
    right = chip_at(lax.rem(pos + 1, n), n) * 2 + core
    left = chip_at(lax.rem(pos + n - 1, n), n) * 2 + core
    partner = chip * 2 + (1 - core)

    own_c = pltpu.make_async_copy(cents_in, buf.at[pl.ds(0, fp), :], local_sem.at[0])
    own_d = pltpu.make_async_copy(docs_in, docs_all.at[0], local_sem.at[1])
    own_i = pltpu.make_async_copy(ids_in, ids_all.at[0], local_sem.at[2])
    own_c.start()
    own_d.start()
    own_i.start()

    barrier = pltpu.get_barrier_semaphore()
    for peer in (left, right, partner):
        pl.semaphore_signal(barrier, inc=1, device_id={"clu": peer}, device_id_type=MESH)
    for k in range(1, nd):
        pl.semaphore_signal(barrier, inc=1, device_id={"doc": lax.rem(doc + k, nd)}, device_id_type=MESH)
    pl.semaphore_wait(barrier, 3 + nd - 1)

    def slot(way, h):
        if h == 0:
            return 0
        if h == hops:
            return n - 1
        return 2 * h - 1 if way == 0 else 2 * h

    def piece(s, m, c):
        return buf.at[pl.ds((2 * s + m) * fp, fp), pl.ds(*chunks[c])]

    def reach(way, c):
        return hops if way == c else hops - 1

    sent = []

    def ring(way, h, c):
        s, t = slot(way, h), slot(way, h + 1)
        copy = pltpu.make_async_remote_copy(
            src_ref=piece(s, 0, c), dst_ref=piece(t, 0, c),
            send_sem=ring_send.at[way, h, c], recv_sem=recv.at[t, 0, c],
            device_id={"clu": right if way == 0 else left}, device_id_type=MESH)
        copy.start()
        sent.append(copy)

    def share(s, c):
        copy = pltpu.make_async_remote_copy(
            src_ref=piece(s, 0, c), dst_ref=piece(s, 1, c),
            send_sem=pair_send.at[s, c], recv_sem=recv.at[s, 1, c],
            device_id={"clu": partner}, device_id_type=MESH)
        copy.start()
        sent.append(copy)

    def landed(s, m, c):
        pltpu.make_async_remote_copy(
            src_ref=piece(s, m, c), dst_ref=piece(s, m, c),
            send_sem=pair_send.at[s, c], recv_sem=recv.at[s, m, c],
            device_id={"clu": partner}, device_id_type=MESH).wait_recv()

    own_c.wait()
    for way, c in ((0, 0), (1, 1), (0, 1), (1, 0)):
        ring(way, 0, c)
    for c in (0, 1):
        share(0, c)
    own_d.wait()
    own_i.wait()
    doc_copies = []
    for k in range(1, nd):
        mate = lax.rem(doc + k, nd)
        for ref, ss, rs in ((ids_all, ids_send, ids_recv), (docs_all, docs_send, docs_recv)):
            copy = pltpu.make_async_remote_copy(
                src_ref=ref.at[0], dst_ref=ref.at[k], send_sem=ss.at[k], recv_sem=rs.at[k],
                device_id={"doc": mate}, device_id_type=MESH)
            copy.start()
            doc_copies.append(copy)

    def owner(s):
        if s == 0:
            p = pos
        elif s == n - 1:
            p = pos + hops
        elif s % 2:
            p = pos + n - (s + 1) // 2
        else:
            p = pos + s // 2
        return chip_at(lax.rem(p, n), n)

    ranges = ((0, n - 3), (n - 3, n - 1), (n - 1, n))
    spread = (dp_a, dp_b, dp_c)

    def permute(k):
        rows = docs_all[k]
        for (first, last), out in zip(ranges, spread):
            wide = out.shape[1]
            lane = lax.broadcasted_iota(jnp.int32, (1, wide), 1)
            target = jnp.full((1, wide), -1, jnp.int32)
            for s in range(first, last):
                chip_s = owner(s)
                for m in (0, 1):
                    part = chip_s * 2 + (core if m == 0 else 1 - core)
                    start = (2 * (s - first) + m) * fp
                    inside = (lane >= start) & (lane < start + feat)
                    target = jnp.where(inside, lane - start + part * feat, target)
            source = lax.broadcasted_iota(jnp.int32, (rows.shape[1], wide), 0)
            mover = jnp.where(source == target, 1.0, 0.0).astype(jnp.bfloat16)
            out[pl.ds(k * rows_dev, rows_dev), :] = jnp.dot(
                rows, mover, preferred_element_type=jnp.float32).astype(jnp.bfloat16)

    def prepare_ids(k):
        base = doc * width
        ids = ids_all[k] - base
        ids = jnp.where((ids >= 0) & (ids < width), ids, -1)
        full = jnp.broadcast_to(ids, (128, rows_dev)).T
        lanes = lax.broadcasted_iota(jnp.int32, (rows_dev, 128), 1)
        idb[pl.ds(k * rows_dev, rows_dev), :] = jnp.where(full >= 0, full - lanes, -(2**20))

    full_tiles, rest = width // TILE, width % TILE

    def phase(index, from_tile, to_tile, with_rest):
        first, last = ranges[index]
        start, depth = 2 * first * fp, 2 * (last - first) * fp
        lhs = spread[index]

        def tile(col, wide):
            block = buf[pl.ds(start, depth), pl.ds(col, wide)]
            prod = jnp.dot(lhs[...], block, preferred_element_type=jnp.float32)
            w32 = block.astype(jnp.float32)
            sq = jnp.sum((w32 * w32).reshape(depth // 8, 8, wide), 0)
            if index == 0:
                acc[:, pl.ds(col, wide)] = prod
                csq[:, pl.ds(col, wide)] = sq
            else:
                acc[:, pl.ds(col, wide)] += prod
                csq[:, pl.ds(col, wide)] += sq

        @pl.loop(from_tile, to_tile)
        def _(t):
            tile(pl.multiple_of(t * TILE, TILE), TILE)

        if with_rest and rest:
            tile(full_tiles * TILE, rest)

    def final_rows(k, make_scale):
        first, last = ranges[2]
        start, depth = 2 * first * fp, 2 * (last - first) * fp
        rs = pl.ds(k * rows_dev, rows_dev)
        mx[rs, :] = jnp.full((rows_dev, 128), -3.0e38, jnp.float32)
        ch[rs, :] = jnp.zeros((rows_dev, 128), jnp.float32)

        def tile(col, wide):
            block = buf[pl.ds(start, depth), pl.ds(col, wide)]
            if make_scale:
                w32 = block.astype(jnp.float32)
                sq = jnp.sum((w32 * w32).reshape(depth // 8, 8, wide), 0) + csq[:, pl.ds(col, wide)]
                sc = lax.rsqrt(jnp.sum(sq, 0, keepdims=True) + epsilon)
                scale[:, pl.ds(col, wide)] = sc
            else:
                sc = scale[:, pl.ds(col, wide)]
            prod = jnp.dot(dp_c[rs, :], block, preferred_element_type=jnp.float32)
            v = (acc[rs, pl.ds(col, wide)] + prod) * sc
            for a in range(0, wide, 128):
                w = min(128, wide - a)
                va = v[:, a:a + w]
                mx[rs, pl.ds(0, w)] = jnp.maximum(mx[rs, pl.ds(0, w)], va)
                hit = idb[rs, pl.ds(0, w)] == col + a
                ch[rs, pl.ds(0, w)] = jnp.where(hit, va, ch[rs, pl.ds(0, w)])

        @pl.loop(0, full_tiles)
        def _(t):
            tile(pl.multiple_of(t * TILE, TILE), TILE)

        if rest:
            tile(full_tiles * TILE, rest)
        best = jnp.max(mx[rs, :].T, 0, keepdims=True)
        chosen = jnp.sum(ch[rs, :].T, 0, keepdims=True)
        return best, chosen

    permute(0)
    prepare_ids(0)
    wide = docs_all[0].astype(jnp.float32)
    squares = wide * wide
    total = squares[:, 0:128]
    for a in range(128, wide.shape[1], 128):
        total = total + squares[:, a:a + 128]
    scale_x = lax.rsqrt(jnp.sum(total.T, 0, keepdims=True) + epsilon)

    def step(way, h, c):
        s = slot(way, h)
        landed(s, 0, c)
        if h < reach(way, c):
            ring(way, h, c)
        share(s, c)

    half_tiles = full_tiles // 2
    for h in range(1, hops):
        last = h == hops - 1
        if last:
            for s in range(n - 3):
                for c in (0, 1):
                    landed(s, 1, c)
            phase(0, 0, half_tiles, False)
        step(0, h, 0)
        step(1, h, 1)
        if last:
            phase(0, half_tiles, full_tiles, True)
        step(0, h, 1)
        step(1, h, 0)
        if h == 1:
            for copy in doc_copies:
                copy.wait()
            for k in range(1, nd):
                permute(k)
                prepare_ids(k)
    for s in (n - 3, n - 2):
        for c in (0, 1):
            landed(s, 1, c)
    phase(1, 0, full_tiles, True)
    for way in (0, 1):
        landed(n - 1, 0, way)
        share(n - 1, way)
    for c in (0, 1):
        landed(n - 1, 1, c)

    returns = []
    for k in range(1, nd):
        best, chosen = final_rows(k, k == 1)
        res[k, 0:1, :] = best
        res[k, 1:2, :] = chosen
        copy = pltpu.make_async_remote_copy(
            src_ref=res.at[k], dst_ref=got.at[k], send_sem=res_send.at[k], recv_sem=res_recv.at[k],
            device_id={"doc": lax.rem(doc + nd - k, nd)}, device_id_type=MESH)
        copy.start()
        returns.append(copy)
    best, chosen = final_rows(0, nd == 1)
    for k in range(1, nd):
        returns[k - 1].wait()
        best = jnp.maximum(best, got[k, 0:1, :])
        chosen = chosen + got[k, 1:2, :]
    near_out[...] = 1.0 - best * scale_x
    chosen_out[...] = 1.0 - chosen * scale_x
    for copy in sent:
        copy.wait_send()


def on_device(docs, centroids, assigned):
    n_clu, nd = lax.axis_size("clu"), lax.axis_size("doc")
    n = n_clu // 2
    rows_dev, depth = docs.shape
    width, feat = centroids.shape
    fp = (feat + 15) // 16 * 16
    cents = centroids.T
    if fp != feat:
        cents = jnp.pad(cents, ((0, fp - feat), (0, 0)))
    rows = nd * rows_dev
    any_space = pl.BlockSpec(memory_space=pl.ANY)
    vmem = pl.BlockSpec(memory_space=pltpu.VMEM)
    dma = pltpu.SemaphoreType.DMA
    hops = n // 2
    line = jax.ShapeDtypeStruct((1, rows_dev), jnp.float32)
    near, chosen = pl.pallas_call(
        functools.partial(kernel, n, nd, feat),
        out_shape=(line, line),
        in_specs=[any_space] * 3,
        out_specs=(vmem, vmem),
        scratch_shapes=[
            pltpu.VMEM((n_clu * fp, width), jnp.bfloat16),
            pltpu.VMEM((nd, rows_dev, depth), jnp.bfloat16),
            pltpu.VMEM((nd, 1, rows_dev), jnp.int32),
            pltpu.VMEM((rows, (n - 3) * 2 * fp), jnp.bfloat16),
            pltpu.VMEM((rows, 4 * fp), jnp.bfloat16),
            pltpu.VMEM((rows, 2 * fp), jnp.bfloat16),
            pltpu.VMEM((rows, width), jnp.float32),
            pltpu.VMEM((rows, 128), jnp.int32),
            pltpu.VMEM((rows, 128), jnp.float32),
            pltpu.VMEM((rows, 128), jnp.float32),
            pltpu.VMEM((8, width), jnp.float32),
            pltpu.VMEM((1, width), jnp.float32),
            pltpu.VMEM((nd, 2, rows_dev), jnp.float32),
            pltpu.VMEM((nd, 2, rows_dev), jnp.float32),
            dma((3,)),
            dma((2, hops, 2)),
            dma((n, 2)),
            dma((n, 2, 2)),
            dma((nd,)), dma((nd,)), dma((nd,)), dma((nd,)), dma((nd,)), dma((nd,)),
        ],
        compiler_params=pltpu.CompilerParams(collective_id=0, has_side_effects=True),
        name="ring_distances",
    )(docs, cents, assigned.reshape(1, rows_dev))
    return near.reshape(rows_dev), chosen.reshape(rows_dev)


def solution(mesh):
    placed = (P(("clu", "doc"), None), P("doc", "clu"), P(("clu", "doc")))
    return jax.shard_map(
        on_device,
        mesh=mesh,
        in_specs=placed,
        out_specs=(P(("clu", "doc")), P(("clu", "doc"))),
        check_vma=False,
    )
```

```python
import functools

import jax
import jax.numpy as jnp
from jax import lax
from jax.experimental import pallas as pl
from jax.experimental.pallas import tpu as pltpu
from jax.sharding import PartitionSpec as P

epsilon = 1e-06
PIECES = 4
ROWS = 64
MESH = pl.DeviceIdType.MESH


def chip_at(pos, n):
    half = n // 2
    return jnp.where(pos < half, 2 * pos, 2 * (n - 1 - pos) + 1)


def cut(width):
    tiles = (width + 127) // 128
    ends = [min(-(-tiles * (c + 1) // PIECES) * 128, width) for c in range(PIECES)]
    return tuple((a, b - a) for a, b in zip([0] + ends[:-1], ends))


def kernel(n, nd, feat, docs_in, cents_in, ids_in, near_out, chosen_out,
           buf, docs_all, ids_all, dp_a, dp_b, dp_c, acc, idb, mx, ch, csq, scale, res, got,
           local_sem, ring_send, pair_send, recv, docs_send, docs_recv, ids_send, ids_recv,
           res_send, res_recv):
    hops = n // 2
    fp = cents_in.shape[0]
    width = cents_in.shape[1]
    rows_dev = docs_in.shape[0]
    chunks = cut(width)
    half = len(chunks) // 2

    clu, doc = lax.axis_index("clu"), lax.axis_index("doc")
    core, chip = lax.rem(clu, 2), lax.div(clu, 2)
    z, x = lax.div(chip, 2), lax.rem(chip, 2)
    pos = jnp.where(x == 0, z, n - 1 - z)
    right = chip_at(lax.rem(pos + 1, n), n) * 2 + core
    left = chip_at(lax.rem(pos + n - 1, n), n) * 2 + core
    partner = chip * 2 + (1 - core)

    own_c = pltpu.make_async_copy(cents_in, buf.at[pl.ds(0, fp), :], local_sem.at[0])
    own_d = pltpu.make_async_copy(docs_in, docs_all.at[0], local_sem.at[1])
    own_i = pltpu.make_async_copy(ids_in, ids_all.at[0], local_sem.at[2])
    own_c.start()
    own_d.start()
    own_i.start()

    barrier = pltpu.get_barrier_semaphore()
    for peer in (left, right, partner):
        pl.semaphore_signal(barrier, inc=1, device_id={"clu": peer}, device_id_type=MESH)
    for k in range(1, nd):
        pl.semaphore_signal(barrier, inc=1, device_id={"doc": lax.rem(doc + k, nd)}, device_id_type=MESH)
    pl.semaphore_wait(barrier, 3 + nd - 1)

    def slot(way, h):
        if h == 0:
            return 0
        if h == hops:
            return n - 1
        return 2 * h - 1 if way == 0 else 2 * h

    def piece(s, m, c):
        return buf.at[pl.ds((2 * s + m) * fp, fp), pl.ds(*chunks[c])]

    def reach(way, c):
        return hops if way == c // half else hops - 1

    sent = []

    def ring(way, h, c):
        s, t = slot(way, h), slot(way, h + 1)
        copy = pltpu.make_async_remote_copy(
            src_ref=piece(s, 0, c), dst_ref=piece(t, 0, c),
            send_sem=ring_send.at[way, h, c], recv_sem=recv.at[t, 0, c],
            device_id={"clu": right if way == 0 else left}, device_id_type=MESH)
        copy.start()
        sent.append(copy)

    def share(s, c):
        copy = pltpu.make_async_remote_copy(
            src_ref=piece(s, 0, c), dst_ref=piece(s, 1, c),
            send_sem=pair_send.at[s, c], recv_sem=recv.at[s, 1, c],
            device_id={"clu": partner}, device_id_type=MESH)
        copy.start()
        sent.append(copy)

    def landed(s, m, c):
        pltpu.make_async_remote_copy(
            src_ref=piece(s, m, c), dst_ref=piece(s, m, c),
            send_sem=pair_send.at[s, c], recv_sem=recv.at[s, m, c],
            device_id={"clu": partner}, device_id_type=MESH).wait_recv()

    own_c.wait()
    for i in range(PIECES):
        ring(0, 0, i)
        ring(1, 0, (i + half) % PIECES)
    for c in range(PIECES):
        share(0, c)
    own_d.wait()
    own_i.wait()
    doc_copies = []
    for k in range(1, nd):
        mate = lax.rem(doc + k, nd)
        for ref, ss, rs in ((ids_all, ids_send, ids_recv), (docs_all, docs_send, docs_recv)):
            copy = pltpu.make_async_remote_copy(
                src_ref=ref.at[0], dst_ref=ref.at[k], send_sem=ss.at[k], recv_sem=rs.at[k],
                device_id={"doc": mate}, device_id_type=MESH)
            copy.start()
            doc_copies.append(copy)

    def owner(s):
        if s == 0:
            p = pos
        elif s == n - 1:
            p = pos + hops
        elif s % 2:
            p = pos + n - (s + 1) // 2
        else:
            p = pos + s // 2
        return chip_at(lax.rem(p, n), n)

    ranges = ((0, n - 3), (n - 3, n - 1), (n - 1, n))
    spread = (dp_a, dp_b, dp_c)

    def permute(k):
        rows = docs_all[k]
        for (first, last), out in zip(ranges, spread):
            wide = out.shape[1]
            lane = lax.broadcasted_iota(jnp.int32, (1, wide), 1)
            target = jnp.full((1, wide), -1, jnp.int32)
            for s in range(first, last):
                chip_s = owner(s)
                for m in (0, 1):
                    part = chip_s * 2 + (core if m == 0 else 1 - core)
                    start = (2 * (s - first) + m) * fp
                    inside = (lane >= start) & (lane < start + feat)
                    target = jnp.where(inside, lane - start + part * feat, target)
            source = lax.broadcasted_iota(jnp.int32, (rows.shape[1], wide), 0)
            mover = jnp.where(source == target, 1.0, 0.0).astype(jnp.bfloat16)
            out[pl.ds(k * rows_dev, rows_dev), :] = jnp.dot(
                rows, mover, preferred_element_type=jnp.float32).astype(jnp.bfloat16)

    def prepare_ids(k):
        base = doc * width
        ids = ids_all[k] - base
        ids = jnp.where((ids >= 0) & (ids < width), ids, -1)
        full = jnp.broadcast_to(ids, (128, rows_dev)).T
        lanes = lax.broadcasted_iota(jnp.int32, (rows_dev, 128), 1)
        idb[pl.ds(k * rows_dev, rows_dev), :] = jnp.where(full >= 0, full - lanes, -(2**20))

    def phase(index, c):
        first, last = ranges[index]
        start, depth = 2 * first * fp, 2 * (last - first) * fp
        cols = pl.ds(*chunks[c])
        block = buf[pl.ds(start, depth), cols]
        prod = jnp.dot(spread[index][...], block, preferred_element_type=jnp.float32)
        w32 = block.astype(jnp.float32)
        sq = jnp.sum((w32 * w32).reshape(depth // 8, 8, chunks[c][1]), 0)
        if index == 0:
            acc[:, cols] = prod
            csq[:, cols] = sq
        else:
            acc[:, cols] += prod
            csq[:, cols] += sq

    tail = pl.ds(2 * (n - 1) * fp, 2 * fp)

    def finish_scale(c):
        cols = pl.ds(*chunks[c])
        w32 = buf[tail, cols].astype(jnp.float32)
        sq = jnp.sum((w32 * w32).reshape(2 * fp // 8, 8, chunks[c][1]), 0) + csq[:, cols]
        scale[:, cols] = lax.rsqrt(jnp.sum(sq, 0, keepdims=True) + epsilon)

    def final(k, c):
        start, wide = chunks[c]
        prod = jnp.dot(dp_c[pl.ds(k * rows_dev, rows_dev), :], buf[tail, pl.ds(start, wide)],
                       preferred_element_type=jnp.float32)
        for r in range(0, rows_dev, ROWS):
            rs = pl.ds(k * rows_dev + r, ROWS)
            top, hit = mx[rs, :], ch[rs, :]
            ids = idb[rs, :]
            for a in range(0, wide, 128):
                w = min(128, wide - a)
                cols = pl.ds(start + a, w)
                v = (acc[rs, cols] + prod[r:r + ROWS, a:a + w]) * scale[:, cols]
                if w == 128:
                    top = jnp.maximum(top, v)
                    hit = jnp.where(ids == start + a, v, hit)
                else:
                    mx[rs, :] = top
                    ch[rs, :] = hit
                    mx[rs, pl.ds(0, w)] = jnp.maximum(mx[rs, pl.ds(0, w)], v)
                    ch[rs, pl.ds(0, w)] = jnp.where(idb[rs, pl.ds(0, w)] == start + a, v, ch[rs, pl.ds(0, w)])
            if wide % 128 == 0:
                mx[rs, :] = top
                ch[rs, :] = hit

    def reduced(k):
        rs = pl.ds(k * rows_dev, rows_dev)
        return (jnp.max(mx[rs, :].T, 0, keepdims=True), jnp.sum(ch[rs, :].T, 0, keepdims=True))

    mx[...] = jnp.full(mx.shape, -3.0e38, jnp.float32)
    ch[...] = jnp.zeros(ch.shape, jnp.float32)
    permute(0)
    prepare_ids(0)
    wide = docs_all[0].astype(jnp.float32)
    squares = wide * wide
    total = squares[:, 0:128]
    for a in range(128, wide.shape[1], 128):
        total = total + squares[:, a:a + 128]
    scale_x = lax.rsqrt(jnp.sum(total.T, 0, keepdims=True) + epsilon)

    def step(way, h, c):
        s = slot(way, h)
        landed(s, 0, c)
        if h < reach(way, c):
            ring(way, h, c)
        share(s, c)

    def pair(h, i):
        step(0, h, i)
        step(1, h, (i + half) % PIECES)

    def partners(slots, c):
        for s in slots:
            landed(s, 1, c)

    early, late = range(n - 3), (n - 3, n - 2)
    order = [j // 2 + half * (j % 2) for j in range(PIECES)]
    for h in range(1, hops):
        for i in range(PIECES):
            pair(h, i)
            if h == hops - 2 and i == half:
                for copy in doc_copies:
                    copy.wait()
                for k in range(1, nd):
                    permute(k)
                    prepare_ids(k)
            if h == hops - 1:
                c = order[i]
                partners(early, c)
                phase(0, c)
    for c in order[:half]:
        partners(late, c)
        phase(1, c)
    for i in range(half):
        for way in (0, 1):
            c = i + half * way
            landed(n - 1, 0, c)
            share(n - 1, c)
    for c in order[half:]:
        partners(late, c)
        phase(1, c)
    for c in order[:-2]:
        landed(n - 1, 1, c)
        finish_scale(c)
        for k in range(nd):
            final(k, c)
    for c in order[-2:]:
        landed(n - 1, 1, c)
        finish_scale(c)

    returns = []
    for k in range(1, nd):
        for c in order[-2:]:
            final(k, c)
        best, chosen = reduced(k)
        res[k, 0:1, :] = best
        res[k, 1:2, :] = chosen
        copy = pltpu.make_async_remote_copy(
            src_ref=res.at[k], dst_ref=got.at[k], send_sem=res_send.at[k], recv_sem=res_recv.at[k],
            device_id={"doc": lax.rem(doc + nd - k, nd)}, device_id_type=MESH)
        copy.start()
        returns.append(copy)
    for c in order[-2:]:
        final(0, c)
    best, chosen = reduced(0)
    for k in range(1, nd):
        returns[k - 1].wait()
        best = jnp.maximum(best, got[k, 0:1, :])
        chosen = chosen + got[k, 1:2, :]
    near_out[...] = best * scale_x
    chosen_out[...] = chosen * scale_x
    for copy in sent:
        copy.wait_send()


def on_device(docs, centroids, assigned):
    n_clu, nd = lax.axis_size("clu"), lax.axis_size("doc")
    n = n_clu // 2
    rows_dev, depth = docs.shape
    width, feat = centroids.shape
    fp = (feat + 15) // 16 * 16
    cents = centroids.T
    if fp != feat:
        cents = jnp.pad(cents, ((0, fp - feat), (0, 0)))
    rows = nd * rows_dev
    any_space = pl.BlockSpec(memory_space=pl.ANY)
    vmem = pl.BlockSpec(memory_space=pltpu.VMEM)
    dma = pltpu.SemaphoreType.DMA
    hops = n // 2
    line = jax.ShapeDtypeStruct((1, rows_dev), jnp.float32)
    near, chosen = pl.pallas_call(
        functools.partial(kernel, n, nd, feat),
        out_shape=(line, line),
        in_specs=[any_space] * 3,
        out_specs=(vmem, vmem),
        scratch_shapes=[
            pltpu.VMEM((n_clu * fp, width), jnp.bfloat16),
            pltpu.VMEM((nd, rows_dev, depth), jnp.bfloat16),
            pltpu.VMEM((nd, 1, rows_dev), jnp.int32),
            pltpu.VMEM((rows, (n - 3) * 2 * fp), jnp.bfloat16),
            pltpu.VMEM((rows, 4 * fp), jnp.bfloat16),
            pltpu.VMEM((rows, 2 * fp), jnp.bfloat16),
            pltpu.VMEM((rows, width), jnp.float32),
            pltpu.VMEM((rows, 128), jnp.int32),
            pltpu.VMEM((rows, 128), jnp.float32),
            pltpu.VMEM((rows, 128), jnp.float32),
            pltpu.VMEM((8, width), jnp.float32),
            pltpu.VMEM((1, width), jnp.float32),
            pltpu.VMEM((nd, 2, rows_dev), jnp.float32),
            pltpu.VMEM((nd, 2, rows_dev), jnp.float32),
            dma((3,)),
            dma((2, hops, PIECES)),
            dma((n, PIECES)),
            dma((n, 2, PIECES)),
            dma((nd,)), dma((nd,)), dma((nd,)), dma((nd,)), dma((nd,)), dma((nd,)),
        ],
        compiler_params=pltpu.CompilerParams(collective_id=0, has_side_effects=True),
        name="ring_distances",
    )(docs, cents, assigned.reshape(1, rows_dev))
    return 1.0 - near.reshape(rows_dev), 1.0 - chosen.reshape(rows_dev)


def solution(mesh):
    placed = (P(("clu", "doc"), None), P("doc", "clu"), P(("clu", "doc")))
    return jax.shard_map(
        on_device,
        mesh=mesh,
        in_specs=placed,
        out_specs=(P(("clu", "doc")), P(("clu", "doc"))),
        check_vma=False,
    )
```
